32 devices in a mesh: grp: 2 (over x), gy: 16 (over z, y, core).
Axes of the slice: x: 2, y: 2, z: 4, core: 2. Of those that a mesh axis runs over, the one named last changes fastest.
Arguments:
- vectors: bfloat16 [512, 2, 3, 16, 512], P('grp', None, None, 'gy'), parts along dimension 0, may hold values from -6 to 6
- gauge_links: bfloat16 [4, 2, 3, 3, 16, 512], P('grp', None, None, None, 'gy'), parts along dimension 0, may hold values from -4 to 4
- perambulators: bfloat16 [32, 4, 2, 2, 256, 256], P('grp', None, None, None, 'gy'), parts along dimension 0, may hold values from -0.25 to 0.25
- momenta: int32 [4, 3], replicated, may hold values from -2 to 2
- path_codes: int32 [2, 2], replicated, may hold values from 0 to 1
- source_times: int32 [8], P('grp'), parts along dimension 0, may hold values from 0 to 15
Outputs:
- contracted: bfloat16 [8, 4, 2, 256, 2, 4, 2, 256], P('grp', None, None, 'gy'), parts along dimension 0
The draws below stay inside these ranges and needn't reach their ends.
There are 2 independent parts, one for each index of `grp`. The reference program is written for one: setup_inputs(seed, part) draws one part's arguments, and reference() takes and returns one part's arrays. A program takes and returns all parts, laid end to end along the dimension named above; an argument that names none is the same for every part. Nothing has to cross between parts.
Inputs may be any that keep to these rules, and one draw needn't show every extreme that they name: `momenta`: momentum components in lattice units.
All inputs are finite; a program needn't handle non-finite values.
Results may differ from the reference program's by a relative error of at most 0.0057.
Values may be sent and summed in bfloat16 or wider, within the bound.
A program may use at most 128 MiB of HBM per device.

```python
import math
import jax
import jax.numpy as jnp
from jax import lax

NVEC = 256
LX = 32
LZ = 16
NMOM = 4
NDISP = 2
NT0 = 16
NSRC = 4
NY = 16
ZX = 512


def set_ends(result, rng, least, top_value):
    longest = result.shape.index(max(result.shape))
    spots = []
    for shift in (0, 1):
        where = [jax.random.randint(jax.random.fold_in(rng, axis), (), 0, length) for axis, length in enumerate(result.shape)]
        where[longest] = (where[longest] + shift) % result.shape[longest]
        spots.append(tuple(where))
    return result.at[spots[0]].set(least).at[spots[1]].set(top_value)


def spiked(drawn, own_key, source, target, blocks, factor):
    owner, partner = [(jnp.arange(drawn.shape[dim]) // (drawn.shape[dim] // blocks)).reshape([-1 if axis == dim else 1 for axis in range(drawn.ndim)]) for dim in (source, target)]
    chosen = jax.random.permutation(own_key, blocks)[partner]
    strong = (owner == chosen) | (owner == (partner + blocks // 2) % blocks)
    return jnp.where(strong, factor * drawn, drawn)


def block_scale(stream_key, extent, shards, low, top_value):
    def one(axis_at, shards_of):
        draws = jax.random.uniform(jax.random.fold_in(jax.random.fold_in(stream_key, 6), axis_at), (shards_of,), jnp.float32, low / len(shards), top_value / len(shards))
        return jnp.repeat(jnp.exp(draws), extent[axis_at] // shards_of).reshape((-1,) + (1,) * (len(extent) - axis_at - 1))

    loudness = one(*shards[0])
    for cut in shards[1:]:
        loudness = loudness * one(*cut)
    return loudness


def gaussian(key, dims, spread, bound, cuts=(), kind=jnp.bfloat16):
    gain = block_scale(key, dims, cuts, -0.22, 0.18) if cuts else 1.0
    drawn = jax.random.normal(key, dims, jnp.float32) * spread * gain
    return jnp.minimum(jnp.maximum(drawn, -bound), bound).astype(kind)


def bell_draw_with(stream_key, shape, deviation, limit, shards, heavy, kind=jnp.bfloat16):
    array = deviation * jax.random.normal(stream_key, shape, jnp.float32)
    if shards:
        array = array * block_scale(stream_key, shape, shards, -0.22, 0.18)
    return jnp.clip(spiked(array, jax.random.fold_in(stream_key, 3), *heavy), -limit, limit).astype(kind)


def setup_inputs(seed: int = 0, part: int = 0) -> dict:
    streams_of = jax.random.split(jax.random.key(seed), 7)
    part_splits = jax.random.split(jax.random.fold_in(streams_of[6], part), 7)
    return {
        "vectors": bell_draw_with(part_splits[0], (NVEC, 2, 3, NY, ZX), 1.0, 6.0, ((3, 16),), (3, 0, 16, 2.0)),
        "gauge_links": gaussian(part_splits[1], (2, 2, 3, 3, NY, ZX), 0.577, 4.0, ((4, 16),)),
        "perambulators": gaussian(part_splits[2], (NT0, 4, 2, 2, NVEC, NVEC), (2 * NVEC) ** -0.5, 0.25, ((4, 16),)),
        "momenta": set_ends(jax.random.randint(streams_of[3], (NMOM, 3), -2, 3), jax.random.fold_in(streams_of[3], 1), -2, 2).astype(jnp.int32),
        "path_codes": set_ends(jax.random.randint(streams_of[4], (NDISP, 2), 0, 2), jax.random.fold_in(streams_of[4], 1), 0, 1).astype(jnp.int32),
        "source_times": set_ends(jax.random.randint(part_splits[5], (NSRC,), 0, NT0), jax.random.fold_in(part_splits[5], 1), 0, NT0 - 1).astype(jnp.int32),
    }


TWO_PI = 6.283185307179586
HIGHEST = lax.Precision.HIGHEST

def color_apply(link_re, link_im, source_re, source_im, dagger):
    if dagger:
        link_re = jnp.swapaxes(link_re, 0, 1)
        link_im = -jnp.swapaxes(link_im, 0, 1)
    real_part = link_re[:, 0][None] * source_re[:, 0][:, None] - link_im[:, 0][None] * source_im[:, 0][:, None]
    imag_part = link_re[:, 0][None] * source_im[:, 0][:, None] + link_im[:, 0][None] * source_re[:, 0][:, None]
    for column in range(1, 3):
        real_part = real_part + link_re[:, column][None] * source_re[:, column][:, None] - link_im[:, column][None] * source_im[:, column][:, None]
        imag_part = imag_part + link_re[:, column][None] * source_im[:, column][:, None] + link_im[:, column][None] * source_re[:, column][:, None]
    return jnp.stack([real_part, imag_part], axis=1)

def link_step(link_data, source_field, dagger):
    return color_apply(link_data[0].astype(jnp.float32), link_data[1].astype(jnp.float32), source_field[:, 0].astype(jnp.float32), source_field[:, 1].astype(jnp.float32), dagger)

def z_step(links_z, source_field, code_value):

    def ahead(field):
        return color_apply(links_z[0], links_z[1], jnp.roll(field[:, 0], -LX, -1), jnp.roll(field[:, 1], -LX, -1), False)

    def behind(field):
        return color_apply(jnp.roll(links_z[0], LX, -1), jnp.roll(links_z[1], LX, -1), jnp.roll(field[:, 0], LX, -1), jnp.roll(field[:, 1], LX, -1), True)
    return lax.cond(code_value == 1, ahead, behind, source_field)

def phase_angles(momenta, y_coord, y_total):
    positions = jnp.arange(LZ * LX, dtype=jnp.int32)
    x_coord = positions % LX
    z_coord = positions // LX
    mom_x = momenta[:, 0][:, None, None]
    mom_y = momenta[:, 1][:, None, None]
    mom_z = momenta[:, 2][:, None, None]
    period = LX * y_total * LZ
    raw_phase = mom_x * x_coord[None, None, :] * (y_total * LZ) + mom_y * y_coord[None, :, None] * (LX * LZ) + mom_z * z_coord[None, None, :] * (LX * y_total)
    residue = jnp.mod(raw_phase, period)
    return residue.astype(jnp.float32) * (TWO_PI / period)

def phased_rows(source_field, angles):
    cosine = jnp.cos(angles)[:, None, None]
    sine_part = jnp.sin(angles)[:, None, None]
    real_in = source_field[None, :, 0]
    imag_in = source_field[None, :, 1]
    stacked = jnp.stack([cosine * real_in + sine_part * imag_in, cosine * imag_in - sine_part * real_in], axis=2)
    return stacked.astype(jnp.bfloat16).reshape(angles.shape[0] * source_field.shape[0], -1)

def conj_rows(vectors):
    vec_count = vectors.shape[0]
    plain_rows = vectors.reshape(vec_count, -1)
    swapped = jnp.concatenate([-vectors[:, 1], vectors[:, 0]], axis=1).reshape(vec_count, -1)
    return jnp.concatenate([plain_rows, swapped], axis=0)

def reference(vectors, gauge_links, perambulators, momenta, path_codes, source_times):
    links_y = gauge_links[0]
    links_z = gauge_links[1].astype(jnp.float32)

    def y_ahead(field):
        return link_step(links_y, jnp.roll(field, -1, axis=3), False)

    def y_behind(field):
        return link_step(jnp.roll(links_y, 1, axis=3), jnp.roll(field, 1, axis=3), True)
    angles = phase_angles(momenta, jnp.arange(NY, dtype=jnp.int32), NY)
    left_rows = conj_rows(vectors).astype(jnp.float32)
    norm_factor = 1.0 / math.sqrt(6 * NY * ZX)
    elementals = []
    for path_index in range(NDISP):
        shifted = lax.cond(path_codes[path_index, 0] == 1, y_ahead, y_behind, vectors)
        shifted = z_step(links_z, shifted, path_codes[path_index, 1])
        right_rows = phased_rows(shifted, angles).astype(jnp.float32)
        partial_value = jnp.dot(left_rows, right_rows.T, precision=HIGHEST)
        elementals.append((partial_value * norm_factor).astype(jnp.bfloat16).reshape(2, NVEC, NMOM, NVEC))
    elemental = jnp.stack(elementals).astype(jnp.float32)
    chosen = perambulators[source_times].astype(jnp.float32)
    pattern = 'sabik,pkmj->sabipmj'
    chosen_re = chosen[:, :, :, 0]
    chosen_im = chosen[:, :, :, 1]
    first = jnp.einsum(pattern, chosen_re, elemental[:, 0], precision=HIGHEST) - jnp.einsum(pattern, chosen_im, elemental[:, 1], precision=HIGHEST)
    second = jnp.einsum(pattern, chosen_re, elemental[:, 1], precision=HIGHEST) + jnp.einsum(pattern, chosen_im, elemental[:, 0], precision=HIGHEST)
    return jnp.stack([first, second], axis=6).astype(jnp.bfloat16)
```

```python
import functools
import math

import jax
import jax.numpy as jnp
from jax import lax
from jax.experimental import pallas as pl
from jax.experimental.pallas import tpu as pltpu
from jax.sharding import PartitionSpec as P

LX = 32
LZ = 16
TWO_PI = 6.283185307179586
MESH = pl.DeviceIdType.MESH
BF = jnp.bfloat16
F32 = jnp.float32


def matmul3(a, b):
    re = jnp.sum(a[0][:, :, None] * b[0][None] - a[1][:, :, None] * b[1][None], axis=1)
    im = jnp.sum(a[0][:, :, None] * b[1][None] + a[1][:, :, None] * b[0][None], axis=1)
    return jnp.stack([re, im])


def dagger(a):
    t = jnp.swapaxes(a, 1, 2)
    return jnp.stack([t[0], -t[1]])


def path_link(link_y, link_z, link_z_up, code):
    forward_y = code[0] == 1
    step_y = jnp.where(forward_y, link_y, dagger(link_y))
    step_z = jnp.where(forward_y, link_z, link_z_up)
    ahead = matmul3(step_z, jnp.roll(step_y, -LX, -1))
    behind = jnp.roll(matmul3(dagger(step_z), step_y), LX, -1)
    return jnp.where(code[1] == 1, ahead, behind)


def phase_angles(momenta, y_coord, y_total):
    positions = jnp.arange(LZ * LX, dtype=jnp.int32)
    x_coord = positions % LX
    z_coord = positions // LX
    period = LX * y_total * LZ
    raw = (
        momenta[:, 0][:, None] * x_coord[None] * (y_total * LZ)
        + momenta[:, 1][:, None] * y_coord * (LX * LZ)
        + momenta[:, 2][:, None] * z_coord[None] * (LX * y_total)
    )
    return jnp.mod(raw, period).astype(F32) * (TWO_PI / period)


def elemental_kernel(codes, links, trig, here, above, out, both, left, rolled, right):
    d = pl.program_id(0)
    nv, width = left.shape[1], left.shape[2]
    sites = width // 6
    moms = right.shape[0]

    @pl.when(d == 0)
    def _():
        both[0] = here[...]
        both[1] = above[...]

    forward_y = codes[d, 0] == 1
    src = jnp.where(forward_y, 1, 0)
    shift = jnp.where(codes[d, 1] == 1, sites - LX, LX)
    rows = 16
    half = width // 2

    @pl.loop(0, nv // rows)
    def _(k):
        at = pl.ds(pl.multiple_of(k * rows, rows), rows)
        whole = both[1 - src, at, :]
        left[0, at, :] = whole
        left[1, at, :] = jnp.concatenate([-whole[:, half:], whole[:, :half]], axis=1)
        for c in range(6):
            piece = both[src, at, c * sites : (c + 1) * sites].astype(F32)
            rolled[at, c * sites : (c + 1) * sites] = pltpu.roll(piece, shift, 1)

    for lt in range(sites // 128):
        lanes = slice(lt * 128, (lt + 1) * 128)
        m = [jnp.broadcast_to(links[0, q : q + 1, lanes], (8, 128)) for q in range(18)]
        tr = [jnp.broadcast_to(trig[0, q : q + 1, lanes], (8, 128)) for q in range(2 * moms)]

        @pl.loop(0, nv // rows)
        def _(k):
            at = pl.ds(pl.multiple_of(k * rows, rows), rows)
            halves = []
            for h in range(2):
                sub = pl.ds(pl.multiple_of(k * rows + 8 * h, 8), 8)
                v = [rolled[sub, c * sites + lt * 128 : c * sites + (lt + 1) * 128] for c in range(6)]
                us = []
                for r in range(3):
                    re = m[3 * r] * v[0] - m[9 + 3 * r] * v[3]
                    im = m[3 * r] * v[3] + m[9 + 3 * r] * v[0]
                    for c in range(1, 3):
                        re = re + m[3 * r + c] * v[c] - m[9 + 3 * r + c] * v[3 + c]
                        im = im + m[3 * r + c] * v[3 + c] + m[9 + 3 * r + c] * v[c]
                    us.append((re, im))
                halves.append(us)
            for p in range(moms):
                for r in range(3):
                    res, ims = [], []
                    for h in range(2):
                        re, im = halves[h][r]
                        res.append(tr[p] * re + tr[moms + p] * im)
                        ims.append(tr[p] * im - tr[moms + p] * re)
                    off = r * sites + lt * 128
                    right[p, at, off : off + 128] = jnp.concatenate(res, axis=0).astype(BF)
                    off = off + half
                    right[p, at, off : off + 128] = jnp.concatenate(ims, axis=0).astype(BF)

    @pl.loop(0, moms)
    def _(p):
        cols = pl.ds(pl.multiple_of(p * nv, nv), nv)
        for c in range(2):
            out[0, c, :, cols] = lax.dot_general(
                left[c], right[p], (((1,), (1,)), ((), ())), preferred_element_type=F32
            ).astype(BF)


def exchange_kernel(chips, norm, partial, full, paired, send, landed, own, sems):
    me = lax.axis_index("gy")
    core = lax.rem(me, 2)
    chip = lax.div(me, 2)
    mate = me + 1 - 2 * core
    mate_core = 1 - core

    def chip_at(k):
        return lax.rem(chip + k, chips)

    barrier = pltpu.get_barrier_semaphore()
    pl.semaphore_signal(barrier, inc=1, device_id={"gy": mate}, device_id_type=MESH)
    for k in range(1, chips):
        pl.semaphore_signal(
            barrier, inc=1, device_id={"gy": 2 * chip_at(k) + core}, device_id_type=MESH
        )
    pl.semaphore_wait(barrier, chips)

    def remote(src, dst, kind, k, target):
        return pltpu.make_async_remote_copy(
            src_ref=src,
            dst_ref=dst,
            send_sem=sems.at[2 * kind, k],
            recv_sem=sems.at[2 * kind + 1, k],
            device_id={"gy": target},
            device_id_type=MESH,
        )

    order = list(range(1, chips)) + [0]
    pairs = []
    for k in order:
        c = chip_at(k)
        copy = remote(partial.at[:, :, 2 * c + mate_core], paired.at[k], 0, k, mate)
        copy.start()
        pairs.append(copy)
    outs = []
    for n, k in enumerate(order):
        pairs[n].wait_recv()
        c = chip_at(k)
        total = partial[:, :, 2 * c + core].astype(F32) + paired[k].astype(F32)
        if k == 0:
            own[...] = total
        else:
            send[k] = total.astype(BF)
            copy = remote(send.at[k], landed.at[k], 1, k, 2 * c + core)
            copy.start()
            outs.append(copy)
    for copy in outs:
        copy.wait_recv()
    total = own[...]
    for k in range(1, chips):
        total = total + landed[k].astype(F32)
    full[:, :, me] = (total * norm).astype(BF)

    gathers = []
    for k in range(1, chips):
        copy = remote(full.at[:, :, me], full.at[:, :, me], 2, k, 2 * chip_at(k) + core)
        copy.start()
        gathers.append(copy)
    copy = remote(full.at[:, :, me], full.at[:, :, me], 3, 0, mate)
    copy.start()
    relays = [copy]
    for k in range(1, chips):
        gathers[k - 1].wait_recv()
        origin = 2 * chip_at(chips - k) + core
        copy = remote(full.at[:, :, origin], full.at[:, :, origin], 3, k, mate)
        copy.start()
        relays.append(copy)
    for copy in relays:
        copy.wait_recv()
    for copy in pairs + outs + gathers + relays:
        copy.wait_send()


def contract_kernel(left, right, out):
    nv = out.shape[5]
    for d in range(out.shape[2]):
        for p in range(out.shape[3]):
            block = jnp.dot(
                left[0], right[d, :, p * nv : (p + 1) * nv], preferred_element_type=F32
            )
            out[0, :, d, p] = block.reshape(-1, 2, nv).astype(BF)


def shards(vectors, gauge_links, perambulators, momenta, path_codes, source_times):
    nv = vectors.shape[0]
    sites = vectors.shape[4]
    size = lax.axis_size("gy")
    y_total = vectors.shape[3] * size
    chips = size // 2
    moms = momenta.shape[0]
    paths = path_codes.shape[0]
    down = [((i + 1) % size, i) for i in range(size)]
    lead = jnp.transpose(vectors, (0, 2, 3, 1, 4))
    lead_up = lax.ppermute(lead, "gy", down)
    links_up = lax.ppermute(gauge_links[1], "gy", down)
    here = jnp.transpose(lead, (0, 3, 1, 2, 4)).reshape(nv, 6 * sites)
    above = jnp.transpose(lead_up, (0, 3, 1, 2, 4)).reshape(nv, 6 * sites)

    link_y = gauge_links[0, :, :, :, 0].astype(F32)
    link_z = gauge_links[1, :, :, :, 0].astype(F32)
    link_z_up = links_up[:, :, :, 0].astype(F32)
    y_here = lax.axis_index("gy")
    links, trig = [], []
    for d in range(paths):
        links.append(path_link(link_y, link_z, link_z_up, path_codes[d]))
        angles = phase_angles(momenta, y_here + jnp.where(path_codes[d, 0] == 1, 0, 1), y_total)
        trig.append(jnp.concatenate([jnp.cos(angles), jnp.sin(angles)]))
    links = jnp.stack(links).reshape(paths, 18, sites)
    trig = jnp.stack(trig)

    partial = pl.pallas_call(
        elemental_kernel,
        grid=(paths,),
        out_shape=jax.ShapeDtypeStruct((paths, 2, nv, moms * nv), BF),
        in_specs=[
            pl.BlockSpec(memory_space=pltpu.SMEM),
            pl.BlockSpec((1, 18, sites), lambda d: (d, 0, 0)),
            pl.BlockSpec((1, 2 * moms, sites), lambda d: (d, 0, 0)),
            pl.BlockSpec((nv, 6 * sites), lambda d: (0, 0)),
            pl.BlockSpec((nv, 6 * sites), lambda d: (0, 0)),
        ],
        out_specs=pl.BlockSpec((1, 2, nv, moms * nv), lambda d: (d, 0, 0, 0)),
        scratch_shapes=[
            pltpu.VMEM((2, nv, 6 * sites), BF),
            pltpu.VMEM((2, nv, 6 * sites), BF),
            pltpu.VMEM((nv, 6 * sites), F32),
            pltpu.VMEM((moms, nv, 6 * sites), BF),
        ],
        compiler_params=pltpu.CompilerParams(vmem_limit_bytes=60 * 2**20),
    )(path_codes, links, trig, here, above)

    rows = nv // size
    norm = 1.0 / math.sqrt(6 * y_total * sites)
    block = (paths, 2, rows, moms * nv)
    gathered = pl.pallas_call(
        functools.partial(exchange_kernel, chips, norm),
        out_shape=jax.ShapeDtypeStruct((paths, 2, size, rows, moms * nv), BF),
        in_specs=[pl.BlockSpec(memory_space=pltpu.VMEM)],
        out_specs=pl.BlockSpec(memory_space=pltpu.VMEM),
        scratch_shapes=[
            pltpu.VMEM((chips,) + block, BF),
            pltpu.VMEM((chips,) + block, BF),
            pltpu.VMEM((chips,) + block, BF),
            pltpu.VMEM(block, F32),
            pltpu.SemaphoreType.DMA((8, chips)),
        ],
        compiler_params=pltpu.CompilerParams(
            collective_id=0, has_side_effects=True, vmem_limit_bytes=60 * 2**20
        ),
    )(partial.reshape(paths, 2, size, rows, moms * nv))
    right = gathered.reshape(paths, 2 * nv, moms * nv)

    chosen = perambulators[source_times]
    times, spins, sources = chosen.shape[:3]
    own = chosen.shape[4]
    re, im = chosen[:, :, :, 0], chosen[:, :, :, 1]
    left = jnp.stack(
        [jnp.concatenate([re, -im], axis=-1), jnp.concatenate([im, re], axis=-1)], axis=4
    ).reshape(times, spins * sources * own * 2, 2 * nv)
    count = spins * sources * own
    out = pl.pallas_call(
        contract_kernel,
        grid=(times,),
        out_shape=jax.ShapeDtypeStruct((times, count, paths, moms, 2, nv), BF),
        in_specs=[
            pl.BlockSpec((1, 2 * count, 2 * nv), lambda s: (s, 0, 0)),
            pl.BlockSpec((paths, 2 * nv, moms * nv), lambda s: (0, 0, 0)),
        ],
        out_specs=pl.BlockSpec((1, count, paths, moms, 2, nv), lambda s: (s, 0, 0, 0, 0, 0)),
        compiler_params=pltpu.CompilerParams(vmem_limit_bytes=60 * 2**20),
    )(left, right)
    return out.reshape(times, spins, sources, own, paths, moms, 2, nv)


def solution(mesh):
    placed = (
        P("grp", None, None, "gy", None),
        P("grp", None, None, None, "gy", None),
        P("grp", None, None, None, "gy", None),
        P(),
        P(),
        P("grp"),
    )
    return jax.shard_map(
        shards,
        mesh=mesh,
        in_specs=placed,
        out_specs=P("grp", None, None, "gy", None, None, None, None),
        check_vma=False,
    )
```

```python
import functools
import math

import jax
import jax.numpy as jnp
from jax import lax
from jax.experimental import pallas as pl
from jax.experimental.pallas import tpu as pltpu
from jax.sharding import PartitionSpec as P

LX = 32
LZ = 16
TWO_PI = 6.283185307179586
MESH = pl.DeviceIdType.MESH
BF = jnp.bfloat16
F32 = jnp.float32


def matmul3(a, b):
    re = jnp.sum(a[0][:, :, None] * b[0][None] - a[1][:, :, None] * b[1][None], axis=1)
    im = jnp.sum(a[0][:, :, None] * b[1][None] + a[1][:, :, None] * b[0][None], axis=1)
    return jnp.stack([re, im])


def dagger(a):
    t = jnp.swapaxes(a, 1, 2)
    return jnp.stack([t[0], -t[1]])


def path_link(link_y, link_z, link_z_up, code):
    forward_y = code[0] == 1
    step_y = jnp.where(forward_y, link_y, dagger(link_y))
    step_z = jnp.where(forward_y, link_z, link_z_up)
    ahead = matmul3(step_z, jnp.roll(step_y, -LX, -1))
    behind = jnp.roll(matmul3(dagger(step_z), step_y), LX, -1)
    return jnp.where(code[1] == 1, ahead, behind)


def phase_angles(momenta, y_coord, y_total):
    positions = jnp.arange(LZ * LX, dtype=jnp.int32)
    x_coord = positions % LX
    z_coord = positions // LX
    period = LX * y_total * LZ
    raw = (
        momenta[:, 0][:, None] * x_coord[None] * (y_total * LZ)
        + momenta[:, 1][:, None] * y_coord * (LX * LZ)
        + momenta[:, 2][:, None] * z_coord[None] * (LX * y_total)
    )
    return jnp.mod(raw, period).astype(F32) * (TWO_PI / period)


def fused_kernel(
    norm, moms, codes, links, trig, here, above, full, both, left, rolled, right,
    part, pair, y_send, y_own, y_pair, z_send, z_land, sems, z_sems,
):
    steps, planes = part.shape[0], part.shape[2]
    rows_own = part.shape[5]
    nv, width = left.shape[1], left.shape[2]
    sites = width // 6
    half = width // 2
    rows = 16
    me = lax.axis_index("gy")
    core = lax.rem(me, 2)
    y = lax.rem(lax.div(me, 2), 2)
    z = lax.div(me, 4)
    mate = me + 1 - 2 * core
    y_mate = me + 2 - 4 * y

    def z_at(k):
        return lax.rem(z + k, planes)

    def z_peer(k):
        return 4 * z_at(k) + 2 * y + core

    barrier = pltpu.get_barrier_semaphore()
    for target in [mate, y_mate] + [z_peer(k) for k in range(1, planes)]:
        pl.semaphore_signal(barrier, inc=1, device_id={"gy": target}, device_id_type=MESH)
    pl.semaphore_wait(barrier, planes + 1)

    def remote(src, dst, pair_sems, target):
        return pltpu.make_async_remote_copy(
            src_ref=src,
            dst_ref=dst,
            send_sem=pair_sems[0],
            recv_sem=pair_sems[1],
            device_id={"gy": target},
            device_id_type=MESH,
        )

    def flat(kind, u):
        return sems.at[2 * kind, u], sems.at[2 * kind + 1, u]

    def along(kind, u, k):
        return z_sems.at[2 * kind, u, k], z_sems.at[2 * kind + 1, u, k]

    def core_copy(u):
        return remote(part.at[u, :, :, :, 1 - core], pair.at[u], flat(0, u), mate)

    def y_copy(u):
        return remote(y_send.at[u], y_pair.at[u], flat(1, u), y_mate)

    def z_copy(u, k):
        return remote(z_send.at[u, :, z_at(k)], z_land.at[u, k], along(0, u, k), z_peer(k))

    def z_gather(u, k):
        ref = full.at[u, :, z, y, core]
        return remote(ref, ref, along(1, u, k), z_peer(k))

    def y_gather(u):
        ref = full.at[u, :, :, y, core]
        return remote(ref, ref, flat(2, u), y_mate)

    def core_gather(u):
        ref = full.at[u, :, :, :, core]
        return remote(ref, ref, flat(3, u), mate)

    both[0] = here[...]
    both[1] = above[...]

    def prepare(d):
        forward_y = codes[d, 0] == 1
        forward_z = codes[d, 1] == 1
        src = jnp.where(forward_y, 1, 0)

        @pl.loop(0, nv // rows)
        def _(k):
            at = pl.ds(pl.multiple_of(k * rows, rows), rows)
            whole = both[1 - src, at, :]
            left[0, at, :] = whole
            left[1, at, :] = jnp.concatenate([-whole[:, half:], whole[:, :half]], axis=1)
            for c in range(6):
                piece = both[src, at, c * sites : (c + 1) * sites].astype(F32)
                rolled[at, c * sites : (c + 1) * sites] = jnp.where(
                    forward_z, pltpu.roll(piece, sites - LX, 1), pltpu.roll(piece, LX, 1)
                )

        for lt in range(sites // 128):
            lanes = slice(lt * 128, (lt + 1) * 128)
            m = [jnp.broadcast_to(links[d, q : q + 1, lanes], (8, 128)) for q in range(18)]
            tr = [jnp.broadcast_to(trig[d, q : q + 1, lanes], (8, 128)) for q in range(2 * moms)]

            @pl.loop(0, nv // rows)
            def _(k):
                at = pl.ds(pl.multiple_of(k * rows, rows), rows)
                halves = []
                for h in range(2):
                    sub = pl.ds(pl.multiple_of(k * rows + 8 * h, 8), 8)
                    v = [
                        rolled[sub, c * sites + lt * 128 : c * sites + (lt + 1) * 128]
                        for c in range(6)
                    ]
                    us = []
                    for r in range(3):
                        re = m[3 * r] * v[0] - m[9 + 3 * r] * v[3]
                        im = m[3 * r] * v[3] + m[9 + 3 * r] * v[0]
                        for c in range(1, 3):
                            re = re + m[3 * r + c] * v[c] - m[9 + 3 * r + c] * v[3 + c]
                            im = im + m[3 * r + c] * v[3 + c] + m[9 + 3 * r + c] * v[c]
                        us.append((re, im))
                    halves.append(us)
                for p in range(moms):
                    for r in range(3):
                        res, ims = [], []
                        for h in range(2):
                            re, im = halves[h][r]
                            res.append(tr[p] * re + tr[moms + p] * im)
                            ims.append(tr[p] * im - tr[moms + p] * re)
                        off = r * sites + lt * 128
                        right[p, at, off : off + 128] = jnp.concatenate(res, axis=0).astype(BF)
                        off = off + half
                        right[p, at, off : off + 128] = jnp.concatenate(ims, axis=0).astype(BF)

    def product(t):
        p = lax.rem(t, moms)
        for c in range(2):
            block = lax.dot_general(
                left[c], right[p], (((1,), (1,)), ((), ())), preferred_element_type=F32
            )
            part[t, c] = block.reshape(planes, 2, 2, rows_own, nv).astype(BF)
        core_copy(t).start()

    def join_cores(u):
        core_copy(u).wait_recv()
        away = part[u, :, :, 1 - y, core].astype(F32) + pair[u, :, :, 1 - y].astype(F32)
        y_send[u] = away.astype(BF)
        y_copy(u).start()
        y_own[u] = part[u, :, :, y, core].astype(F32) + pair[u, :, :, y].astype(F32)

    def join_y(u):
        y_copy(u).wait_recv()
        total = y_own[u] + y_pair[u].astype(F32)
        y_own[u] = total
        z_send[u] = total.astype(BF)
        for k in range(1, planes):
            z_copy(u, k).start()

    def join_z(u):
        for k in range(1, planes):
            z_copy(u, k).wait_recv()
        total = y_own[u, :, z]
        for k in range(1, planes):
            total = total + z_land[u, k].astype(F32)
        full[u, :, z, y, core] = (total * norm).astype(BF)
        for k in range(1, planes):
            z_gather(u, k).start()

    def share_y(u):
        for k in range(1, planes):
            z_gather(u, k).wait_recv()
        y_gather(u).start()

    def share_core(u):
        y_gather(u).wait_recv()
        core_gather(u).start()

    def finish(u):
        core_gather(u).wait()
        core_copy(u).wait_send()
        y_copy(u).wait_send()
        y_gather(u).wait_send()
        for k in range(1, planes):
            z_copy(u, k).wait_send()
            z_gather(u, k).wait_send()

    stages = [product, join_cores, join_y, join_z, share_y, share_core, finish]

    @pl.loop(0, steps + len(stages) - 1)
    def _(t):
        @pl.when(jnp.logical_and(t < steps, lax.rem(t, moms) == 0))
        def _():
            prepare(lax.div(t, moms))

        for lag, stage in enumerate(stages):
            @pl.when(jnp.logical_and(t >= lag, t - lag < steps))
            def _():
                stage(t - lag)


def contract_kernel(left, right, out):
    nv = out.shape[5]
    for d in range(out.shape[2]):
        for p in range(out.shape[3]):
            block = jnp.dot(
                left[0], right[d * out.shape[3] + p], preferred_element_type=F32
            )
            out[0, :, d, p] = block.reshape(-1, 2, nv).astype(BF)


def shards(vectors, gauge_links, perambulators, momenta, path_codes, source_times):
    nv = vectors.shape[0]
    sites = vectors.shape[4]
    size = lax.axis_size("gy")
    y_total = vectors.shape[3] * size
    moms = momenta.shape[0]
    paths = path_codes.shape[0]
    down = [((i + 1) % size, i) for i in range(size)]
    lead = jnp.transpose(vectors, (0, 2, 3, 1, 4))
    lead_up = lax.ppermute(lead, "gy", down)
    links_up = lax.ppermute(gauge_links[1], "gy", down)
    here = jnp.transpose(lead, (0, 3, 1, 2, 4)).reshape(nv, 6 * sites)
    above = jnp.transpose(lead_up, (0, 3, 1, 2, 4)).reshape(nv, 6 * sites)

    link_y = gauge_links[0, :, :, :, 0].astype(F32)
    link_z = gauge_links[1, :, :, :, 0].astype(F32)
    link_z_up = links_up[:, :, :, 0].astype(F32)
    y_here = lax.axis_index("gy")
    links, trig = [], []
    for d in range(paths):
        links.append(path_link(link_y, link_z, link_z_up, path_codes[d]))
        angles = phase_angles(momenta, y_here + jnp.where(path_codes[d, 0] == 1, 0, 1), y_total)
        trig.append(jnp.concatenate([jnp.cos(angles), jnp.sin(angles)]))
    links = jnp.stack(links).reshape(paths, 18, sites)
    trig = jnp.stack(trig)

    rows = nv // size
    steps, planes = paths * moms, size // 4
    norm = 1.0 / math.sqrt(6 * y_total * sites)
    vmem = pl.BlockSpec(memory_space=pltpu.VMEM)
    right = pl.pallas_call(
        functools.partial(fused_kernel, norm, moms),
        out_shape=jax.ShapeDtypeStruct((steps, 2, planes, 2, 2, rows, nv), BF),
        in_specs=[pl.BlockSpec(memory_space=pltpu.SMEM), vmem, vmem, vmem, vmem],
        out_specs=vmem,
        scratch_shapes=[
            pltpu.VMEM((2, nv, 6 * sites), BF),
            pltpu.VMEM((2, nv, 6 * sites), BF),
            pltpu.VMEM((nv, 6 * sites), F32),
            pltpu.VMEM((moms, nv, 6 * sites), BF),
            pltpu.VMEM((steps, 2, planes, 2, 2, rows, nv), BF),
            pltpu.VMEM((steps, 2, planes, 2, rows, nv), BF),
            pltpu.VMEM((steps, 2, planes, rows, nv), BF),
            pltpu.VMEM((steps, 2, planes, rows, nv), F32),
            pltpu.VMEM((steps, 2, planes, rows, nv), BF),
            pltpu.VMEM((steps, 2, planes, rows, nv), BF),
            pltpu.VMEM((steps, planes, 2, rows, nv), BF),
            pltpu.SemaphoreType.DMA((8, steps)),
            pltpu.SemaphoreType.DMA((4, steps, planes)),
        ],
        compiler_params=pltpu.CompilerParams(
            collective_id=0, has_side_effects=True, vmem_limit_bytes=60 * 2**20
        ),
    )(path_codes, links, trig, here, above).reshape(steps, 2 * nv, nv)

    chosen = perambulators[source_times]
    times, spins, sources = chosen.shape[:3]
    own = chosen.shape[4]
    re, im = chosen[:, :, :, 0], chosen[:, :, :, 1]
    left = jnp.stack(
        [jnp.concatenate([re, -im], axis=-1), jnp.concatenate([im, re], axis=-1)], axis=4
    ).reshape(times, spins * sources * own * 2, 2 * nv)
    count = spins * sources * own
    out = pl.pallas_call(
        contract_kernel,
        grid=(times,),
        out_shape=jax.ShapeDtypeStruct((times, count, paths, moms, 2, nv), BF),
        in_specs=[
            pl.BlockSpec((1, 2 * count, 2 * nv), lambda s: (s, 0, 0)),
            pl.BlockSpec((steps, 2 * nv, nv), lambda s: (0, 0, 0)),
        ],
        out_specs=pl.BlockSpec((1, count, paths, moms, 2, nv), lambda s: (s, 0, 0, 0, 0, 0)),
        compiler_params=pltpu.CompilerParams(vmem_limit_bytes=60 * 2**20),
    )(left, right)
    return out.reshape(times, spins, sources, own, paths, moms, 2, nv)


def solution(mesh):
    placed = (
        P("grp", None, None, "gy", None),
        P("grp", None, None, None, "gy", None),
        P("grp", None, None, None, "gy", None),
        P(),
        P(),
        P("grp"),
    )
    return jax.shard_map(
        shards,
        mesh=mesh,
        in_specs=placed,
        out_specs=P("grp", None, None, "gy", None, None, None, None),
        check_vma=False,
    )
```

```python
import functools
import math

import jax
import jax.numpy as jnp
from jax import lax
from jax.experimental import pallas as pl
from jax.experimental.pallas import tpu as pltpu
from jax.sharding import PartitionSpec as P

LX = 32
LZ = 16
TWO_PI = 6.283185307179586
MESH = pl.DeviceIdType.MESH
BF = jnp.bfloat16
F32 = jnp.float32


def matmul3(a, b):
    re = jnp.sum(a[0][:, :, None] * b[0][None] - a[1][:, :, None] * b[1][None], axis=1)
    im = jnp.sum(a[0][:, :, None] * b[1][None] + a[1][:, :, None] * b[0][None], axis=1)
    return jnp.stack([re, im])


def dagger(a):
    t = jnp.swapaxes(a, 1, 2)
    return jnp.stack([t[0], -t[1]])


def path_link(link_y, link_z, link_z_up, code):
    forward_y = code[0] == 1
    step_y = jnp.where(forward_y, link_y, dagger(link_y))
    step_z = jnp.where(forward_y, link_z, link_z_up)
    ahead = matmul3(step_z, jnp.roll(step_y, -LX, -1))
    behind = jnp.roll(matmul3(dagger(step_z), step_y), LX, -1)
    return jnp.where(code[1] == 1, ahead, behind)


def phase_angles(momenta, y_coord, y_total):
    positions = jnp.arange(LZ * LX, dtype=jnp.int32)
    x_coord = positions % LX
    z_coord = positions // LX
    period = LX * y_total * LZ
    raw = (
        momenta[:, 0][:, None] * x_coord[None] * (y_total * LZ)
        + momenta[:, 1][:, None] * y_coord * (LX * LZ)
        + momenta[:, 2][:, None] * z_coord[None] * (LX * y_total)
    )
    return jnp.mod(raw, period).astype(F32) * (TWO_PI / period)


def fused_kernel(
    norm, moms, codes, links, trig, here, above, full, both, left, rolled, right,
    part, pair, y_send, y_own, y_pair, z_send, z_land, sems, z_sems,
):
    steps, planes = part.shape[0], part.shape[2]
    rows_own = part.shape[5]
    nv, width = left.shape[1], left.shape[2]
    sites = width // 6
    half = width // 2
    rows = 16
    me = lax.axis_index("gy")
    core = lax.rem(me, 2)
    y = lax.rem(lax.div(me, 2), 2)
    z = lax.div(me, 4)
    mate = me + 1 - 2 * core
    y_mate = me + 2 - 4 * y

    def z_at(k):
        return lax.rem(z + k, planes)

    def z_peer(k):
        return 4 * z_at(k) + 2 * y + core

    barrier = pltpu.get_barrier_semaphore()
    for target in [mate, y_mate] + [z_peer(k) for k in range(1, planes)]:
        pl.semaphore_signal(barrier, inc=1, device_id={"gy": target}, device_id_type=MESH)
    pl.semaphore_wait(barrier, planes + 1)

    def remote(src, dst, pair_sems, target):
        return pltpu.make_async_remote_copy(
            src_ref=src,
            dst_ref=dst,
            send_sem=pair_sems[0],
            recv_sem=pair_sems[1],
            device_id={"gy": target},
            device_id_type=MESH,
        )

    def flat(kind, u):
        return sems.at[2 * kind, u], sems.at[2 * kind + 1, u]

    def along(kind, u, k):
        return z_sems.at[2 * kind, u, k], z_sems.at[2 * kind + 1, u, k]

    def core_copy(u):
        return remote(part.at[u, :, :, :, 1 - core], pair.at[u], flat(0, u), mate)

    def y_copy(u):
        return remote(y_send.at[u], y_pair.at[u], flat(1, u), y_mate)

    def z_copy(u, k):
        return remote(z_send.at[u, :, z_at(k)], z_land.at[u, k], along(0, u, k), z_peer(k))

    def z_gather(u, k):
        ref = full.at[u, :, z, y, core]
        return remote(ref, ref, along(1, u, k), z_peer(k))

    def y_gather(u):
        ref = full.at[u, :, :, y, core]
        return remote(ref, ref, flat(2, u), y_mate)

    def core_gather(u):
        ref = full.at[u, :, :, :, core]
        return remote(ref, ref, flat(3, u), mate)

    both[0] = here[...]
    both[1] = above[...]

    def prepare(d):
        forward_y = codes[d, 0] == 1
        forward_z = codes[d, 1] == 1
        src = jnp.where(forward_y, 1, 0)

        @pl.loop(0, nv // rows)
        def _(k):
            at = pl.ds(pl.multiple_of(k * rows, rows), rows)
            whole = both[1 - src, at, :]
            left[0, at, :] = whole
            left[1, at, :] = jnp.concatenate([-whole[:, half:], whole[:, :half]], axis=1)
            for c in range(6):
                piece = both[src, at, c * sites : (c + 1) * sites].astype(F32)
                rolled[at, c * sites : (c + 1) * sites] = jnp.where(
                    forward_z, pltpu.roll(piece, sites - LX, 1), pltpu.roll(piece, LX, 1)
                )

        for lt in range(sites // 128):
            lanes = slice(lt * 128, (lt + 1) * 128)
            m = [jnp.broadcast_to(links[d, q : q + 1, lanes], (8, 128)) for q in range(18)]
            tr = [jnp.broadcast_to(trig[d, q : q + 1, lanes], (8, 128)) for q in range(2 * moms)]

            @pl.loop(0, nv // rows)
            def _(k):
                at = pl.ds(pl.multiple_of(k * rows, rows), rows)
                halves = []
                for h in range(2):
                    sub = pl.ds(pl.multiple_of(k * rows + 8 * h, 8), 8)
                    v = [
                        rolled[sub, c * sites + lt * 128 : c * sites + (lt + 1) * 128]
                        for c in range(6)
                    ]
                    us = []
                    for r in range(3):
                        re = m[3 * r] * v[0] - m[9 + 3 * r] * v[3]
                        im = m[3 * r] * v[3] + m[9 + 3 * r] * v[0]
                        for c in range(1, 3):
                            re = re + m[3 * r + c] * v[c] - m[9 + 3 * r + c] * v[3 + c]
                            im = im + m[3 * r + c] * v[3 + c] + m[9 + 3 * r + c] * v[c]
                        us.append((re, im))
                    halves.append(us)
                for p in range(moms):
                    for r in range(3):
                        res, ims = [], []
                        for h in range(2):
                            re, im = halves[h][r]
                            res.append(tr[p] * re + tr[moms + p] * im)
                            ims.append(tr[p] * im - tr[moms + p] * re)
                        off = r * sites + lt * 128
                        right[p, at, off : off + 128] = jnp.concatenate(res, axis=0).astype(BF)
                        off = off + half
                        right[p, at, off : off + 128] = jnp.concatenate(ims, axis=0).astype(BF)

    def product(t):
        p = lax.rem(t, moms)
        for c in range(2):
            block = lax.dot_general(
                left[c], right[p], (((1,), (1,)), ((), ())), preferred_element_type=F32
            )
            part[t, c] = block.reshape(planes, 2, 2, rows_own, nv).astype(BF)
        core_copy(t).start()

    def join_cores(u):
        core_copy(u).wait_recv()
        away = part[u, :, :, 1 - y, core].astype(F32) + pair[u, :, :, 1 - y].astype(F32)
        y_send[u] = away.astype(BF)
        y_copy(u).start()
        y_own[u] = part[u, :, :, y, core].astype(F32) + pair[u, :, :, y].astype(F32)

    def join_y(u):
        y_copy(u).wait_recv()
        total = y_own[u] + y_pair[u].astype(F32)
        y_own[u] = total
        z_send[u] = total.astype(BF)
        for k in range(1, planes):
            z_copy(u, k).start()

    def join_z(u):
        for k in range(1, planes):
            z_copy(u, k).wait_recv()
        total = y_own[u, :, z]
        for k in range(1, planes):
            total = total + z_land[u, k].astype(F32)
        full[u, :, z, y, core] = (total * norm).astype(BF)
        for k in range(1, planes):
            z_gather(u, k).start()

    def share_y(u):
        for k in range(1, planes):
            z_gather(u, k).wait_recv()
        y_gather(u).start()

    def share_core(u):
        y_gather(u).wait_recv()
        core_gather(u).start()

    def finish(u):
        core_gather(u).wait()
        core_copy(u).wait_send()
        y_copy(u).wait_send()
        y_gather(u).wait_send()
        for k in range(1, planes):
            z_copy(u, k).wait_send()
            z_gather(u, k).wait_send()

    stages = [
        (product, 0), (join_cores, 1), (join_y, 3), (join_z, 5),
        (share_y, 7), (share_core, 9), (finish, 10),
    ]
    prepare(0)

    @pl.loop(0, steps + stages[-1][1])
    def _(t):
        for stage, lag in stages:
            @pl.when(jnp.logical_and(t >= lag, t - lag < steps))
            def _():
                stage(t - lag)

        @pl.when(jnp.logical_and(t < steps - 1, lax.rem(t + 1, moms) == 0))
        def _():
            prepare(lax.div(t + 1, moms))


def contract_kernel(left, right, out):
    nv = out.shape[5]
    for d in range(out.shape[2]):
        for p in range(out.shape[3]):
            block = jnp.dot(
                left[0], right[d * out.shape[3] + p], preferred_element_type=F32
            )
            out[0, :, d, p] = block.reshape(-1, 2, nv).astype(BF)


def shards(vectors, gauge_links, perambulators, momenta, path_codes, source_times):
    nv = vectors.shape[0]
    sites = vectors.shape[4]
    size = lax.axis_size("gy")
    y_total = vectors.shape[3] * size
    moms = momenta.shape[0]
    paths = path_codes.shape[0]
    down = [((i + 1) % size, i) for i in range(size)]
    lead = jnp.transpose(vectors, (0, 2, 3, 1, 4))
    lead_up = lax.ppermute(lead, "gy", down)
    links_up = lax.ppermute(gauge_links[1], "gy", down)
    here = jnp.transpose(lead, (0, 3, 1, 2, 4)).reshape(nv, 6 * sites)
    above = jnp.transpose(lead_up, (0, 3, 1, 2, 4)).reshape(nv, 6 * sites)

    link_y = gauge_links[0, :, :, :, 0].astype(F32)
    link_z = gauge_links[1, :, :, :, 0].astype(F32)
    link_z_up = links_up[:, :, :, 0].astype(F32)
    y_here = lax.axis_index("gy")
    links, trig = [], []
    for d in range(paths):
        links.append(path_link(link_y, link_z, link_z_up, path_codes[d]))
        angles = phase_angles(momenta, y_here + jnp.where(path_codes[d, 0] == 1, 0, 1), y_total)
        trig.append(jnp.concatenate([jnp.cos(angles), jnp.sin(angles)]))
    links = jnp.stack(links).reshape(paths, 18, sites)
    trig = jnp.stack(trig)

    rows = nv // size
    steps, planes = paths * moms, size // 4
    norm = 1.0 / math.sqrt(6 * y_total * sites)
    vmem = pl.BlockSpec(memory_space=pltpu.VMEM)
    right = pl.pallas_call(
        functools.partial(fused_kernel, norm, moms),
        out_shape=jax.ShapeDtypeStruct((steps, 2, planes, 2, 2, rows, nv), BF),
        in_specs=[pl.BlockSpec(memory_space=pltpu.SMEM), vmem, vmem, vmem, vmem],
        out_specs=vmem,
        scratch_shapes=[
            pltpu.VMEM((2, nv, 6 * sites), BF),
            pltpu.VMEM((2, nv, 6 * sites), BF),
            pltpu.VMEM((nv, 6 * sites), F32),
            pltpu.VMEM((moms, nv, 6 * sites), BF),
            pltpu.VMEM((steps, 2, planes, 2, 2, rows, nv), BF),
            pltpu.VMEM((steps, 2, planes, 2, rows, nv), BF),
            pltpu.VMEM((steps, 2, planes, rows, nv), BF),
            pltpu.VMEM((steps, 2, planes, rows, nv), F32),
            pltpu.VMEM((steps, 2, planes, rows, nv), BF),
            pltpu.VMEM((steps, 2, planes, rows, nv), BF),
            pltpu.VMEM((steps, planes, 2, rows, nv), BF),
            pltpu.SemaphoreType.DMA((8, steps)),
            pltpu.SemaphoreType.DMA((4, steps, planes)),
        ],
        compiler_params=pltpu.CompilerParams(
            collective_id=0, has_side_effects=True, vmem_limit_bytes=60 * 2**20
        ),
    )(path_codes, links, trig, here, above).reshape(steps, 2 * nv, nv)

    chosen = perambulators[source_times]
    times, spins, sources = chosen.shape[:3]
    own = chosen.shape[4]
    re, im = chosen[:, :, :, 0], chosen[:, :, :, 1]
    left = jnp.stack(
        [jnp.concatenate([re, -im], axis=-1), jnp.concatenate([im, re], axis=-1)], axis=4
    ).reshape(times, spins * sources * own * 2, 2 * nv)
    count = spins * sources * own
    out = pl.pallas_call(
        contract_kernel,
        grid=(times,),
        out_shape=jax.ShapeDtypeStruct((times, count, paths, moms, 2, nv), BF),
        in_specs=[
            pl.BlockSpec((1, 2 * count, 2 * nv), lambda s: (s, 0, 0)),
            pl.BlockSpec((steps, 2 * nv, nv), lambda s: (0, 0, 0)),
        ],
        out_specs=pl.BlockSpec((1, count, paths, moms, 2, nv), lambda s: (s, 0, 0, 0, 0, 0)),
        compiler_params=pltpu.CompilerParams(vmem_limit_bytes=60 * 2**20),
    )(left, right)
    return out.reshape(times, spins, sources, own, paths, moms, 2, nv)


def solution(mesh):
    placed = (
        P("grp", None, None, "gy", None),
        P("grp", None, None, None, "gy", None),
        P("grp", None, None, None, "gy", None),
        P(),
        P(),
        P("grp"),
    )
    return jax.shard_map(
        shards,
        mesh=mesh,
        in_specs=placed,
        out_specs=P("grp", None, None, "gy", None, None, None, None),
        check_vma=False,
    )
```

```python
import functools
import math

import jax
import jax.numpy as jnp
from jax import lax
from jax.experimental import pallas as pl
from jax.experimental.pallas import tpu as pltpu
from jax.sharding import PartitionSpec as P

LX = 32
LZ = 16
TWO_PI = 6.283185307179586
MESH = pl.DeviceIdType.MESH
BF = jnp.bfloat16
F32 = jnp.float32


def matmul3(a, b):
    re = jnp.sum(a[0][:, :, None] * b[0][None] - a[1][:, :, None] * b[1][None], axis=1)
    im = jnp.sum(a[0][:, :, None] * b[1][None] + a[1][:, :, None] * b[0][None], axis=1)
    return jnp.stack([re, im])


def dagger(a):
    t = jnp.swapaxes(a, 1, 2)
    return jnp.stack([t[0], -t[1]])


def path_link(link_y, link_z, link_z_up, code):
    forward_y = code[0] == 1
    step_y = jnp.where(forward_y, link_y, dagger(link_y))
    step_z = jnp.where(forward_y, link_z, link_z_up)
    ahead = matmul3(step_z, jnp.roll(step_y, -LX, -1))
    behind = jnp.roll(matmul3(dagger(step_z), step_y), LX, -1)
    return jnp.where(code[1] == 1, ahead, behind)


def phase_angles(momenta, y_coord, y_total):
    positions = jnp.arange(LZ * LX, dtype=jnp.int32)
    x_coord = positions % LX
    z_coord = positions // LX
    period = LX * y_total * LZ
    raw = (
        momenta[:, 0][:, None] * x_coord[None] * (y_total * LZ)
        + momenta[:, 1][:, None] * y_coord * (LX * LZ)
        + momenta[:, 2][:, None] * z_coord[None] * (LX * y_total)
    )
    return jnp.mod(raw, period).astype(F32) * (TWO_PI / period)


def fused_kernel(
    norm, moms, codes, links, trig, here, above, full, both, left, rolled, right,
    part, pair, y_send, y_own, y_pair, z_send, z_land, sems, z_sems,
):
    steps, planes = part.shape[0], part.shape[2]
    rows_own = part.shape[5]
    nv, width = left.shape[1], left.shape[2]
    sites = width // 6
    half = width // 2
    rows = 16
    me = lax.axis_index("gy")
    core = lax.rem(me, 2)
    y = lax.rem(lax.div(me, 2), 2)
    z = lax.div(me, 4)
    mate = me + 1 - 2 * core
    y_mate = me + 2 - 4 * y

    def z_at(k):
        return lax.rem(z + k, planes)

    def z_peer(k):
        return 4 * z_at(k) + 2 * y + core

    barrier = pltpu.get_barrier_semaphore()
    for target in [mate, y_mate] + [z_peer(k) for k in range(1, planes)]:
        pl.semaphore_signal(barrier, inc=1, device_id={"gy": target}, device_id_type=MESH)
    pl.semaphore_wait(barrier, planes + 1)

    def remote(src, dst, pair_sems, target):
        return pltpu.make_async_remote_copy(
            src_ref=src,
            dst_ref=dst,
            send_sem=pair_sems[0],
            recv_sem=pair_sems[1],
            device_id={"gy": target},
            device_id_type=MESH,
        )

    def flat(kind, u):
        return sems.at[2 * kind, u], sems.at[2 * kind + 1, u]

    def along(kind, u, k):
        return z_sems.at[2 * kind, u, k], z_sems.at[2 * kind + 1, u, k]

    def core_copy(u):
        return remote(part.at[u, :, :, :, 1 - core], pair.at[u], flat(0, u), mate)

    def y_copy(u):
        return remote(y_send.at[u], y_pair.at[u], flat(1, u), y_mate)

    def z_copy(u, k):
        return remote(z_send.at[u, :, z_at(k)], z_land.at[u, k], along(0, u, k), z_peer(k))

    def z_gather(u, k):
        ref = full.at[u, :, z, y, core]
        return remote(ref, ref, along(1, u, k), z_peer(k))

    def y_gather(u):
        ref = full.at[u, :, :, y, core]
        return remote(ref, ref, flat(2, u), y_mate)

    def core_gather(u):
        ref = full.at[u, :, :, :, core]
        return remote(ref, ref, flat(3, u), mate)

    both[0] = here[...]
    both[1] = above[...]

    def prepare(d):
        forward_y = codes[d, 0] == 1
        forward_z = codes[d, 1] == 1
        src = jnp.where(forward_y, 1, 0)

        @pl.loop(0, nv // rows)
        def _(k):
            at = pl.ds(pl.multiple_of(k * rows, rows), rows)
            whole = both[1 - src, at, :]
            left[0, at, :] = whole
            left[1, at, :] = jnp.concatenate([-whole[:, half:], whole[:, :half]], axis=1)
            for c in range(6):
                piece = both[src, at, c * sites : (c + 1) * sites].astype(F32)
                rolled[at, c * sites : (c + 1) * sites] = jnp.where(
                    forward_z, pltpu.roll(piece, sites - LX, 1), pltpu.roll(piece, LX, 1)
                )

        for lt in range(sites // 128):
            lanes = slice(lt * 128, (lt + 1) * 128)
            m = [jnp.broadcast_to(links[d, q : q + 1, lanes], (8, 128)) for q in range(18)]
            tr = [jnp.broadcast_to(trig[d, q : q + 1, lanes], (8, 128)) for q in range(2 * moms)]

            @pl.loop(0, nv // rows)
            def _(k):
                at = pl.ds(pl.multiple_of(k * rows, rows), rows)
                halves = []
                for h in range(2):
                    sub = pl.ds(pl.multiple_of(k * rows + 8 * h, 8), 8)
                    v = [
                        rolled[sub, c * sites + lt * 128 : c * sites + (lt + 1) * 128]
                        for c in range(6)
                    ]
                    us = []
                    for r in range(3):
                        re = m[3 * r] * v[0] - m[9 + 3 * r] * v[3]
                        im = m[3 * r] * v[3] + m[9 + 3 * r] * v[0]
                        for c in range(1, 3):
                            re = re + m[3 * r + c] * v[c] - m[9 + 3 * r + c] * v[3 + c]
                            im = im + m[3 * r + c] * v[3 + c] + m[9 + 3 * r + c] * v[c]
                        us.append((re, im))
                    halves.append(us)
                for p in range(moms):
                    for r in range(3):
                        res, ims = [], []
                        for h in range(2):
                            re, im = halves[h][r]
                            res.append(tr[p] * re + tr[moms + p] * im)
                            ims.append(tr[p] * im - tr[moms + p] * re)
                        off = r * sites + lt * 128
                        right[p, at, off : off + 128] = jnp.concatenate(res, axis=0).astype(BF)
                        off = off + half
                        right[p, at, off : off + 128] = jnp.concatenate(ims, axis=0).astype(BF)

    def product(t):
        p = lax.rem(t, moms)
        for c in range(2):
            block = lax.dot_general(
                left[c], right[p], (((1,), (1,)), ((), ())), preferred_element_type=F32
            )
            part[t, c] = block.reshape(planes, 2, 2, rows_own, nv).astype(BF)
        core_copy(t).start()

    def join_cores(u):
        core_copy(u).wait_recv()
        away = part[u, :, :, 1 - y, core].astype(F32) + pair[u, :, :, 1 - y].astype(F32)
        y_send[u] = away.astype(BF)
        y_copy(u).start()
        y_own[u] = part[u, :, :, y, core].astype(F32) + pair[u, :, :, y].astype(F32)

    def join_y(u):
        y_copy(u).wait_recv()
        total = y_own[u] + y_pair[u].astype(F32)
        y_own[u] = total
        z_send[u] = total.astype(BF)
        for k in range(1, planes):
            z_copy(u, k).start()

    def join_z(u):
        for k in range(1, planes):
            z_copy(u, k).wait_recv()
        total = y_own[u, :, z]
        for k in range(1, planes):
            total = total + z_land[u, k].astype(F32)
        full[u, :, z, y, core] = (total * norm).astype(BF)
        for k in range(1, planes):
            z_gather(u, k).start()

    def share_y(u):
        for k in range(1, planes):
            z_gather(u, k).wait_recv()
        y_gather(u).start()

    def share_core(u):
        y_gather(u).wait_recv()
        core_gather(u).start()

    def finish(u):
        core_gather(u).wait()
        core_copy(u).wait_send()
        y_copy(u).wait_send()
        y_gather(u).wait_send()
        for k in range(1, planes):
            z_copy(u, k).wait_send()
            z_gather(u, k).wait_send()

    stages = [
        (product, 0), (join_cores, 1), (join_y, 4), (join_z, 7),
        (share_y, 10), (share_core, 13), (finish, 14),
    ]
    prepare(0)

    @pl.loop(0, steps + stages[-1][1])
    def _(t):
        for stage, lag in stages:
            @pl.when(jnp.logical_and(t >= lag, t - lag < steps))
            def _():
                stage(t - lag)

        @pl.when(jnp.logical_and(t < steps - 1, lax.rem(t + 1, moms) == 0))
        def _():
            prepare(lax.div(t + 1, moms))


def contract_kernel(left, right, out):
    nv = out.shape[5]
    for d in range(out.shape[2]):
        for p in range(out.shape[3]):
            block = jnp.dot(
                left[0], right[d * out.shape[3] + p], preferred_element_type=F32
            )
            out[0, :, d, p] = block.reshape(-1, 2, nv).astype(BF)


def shards(vectors, gauge_links, perambulators, momenta, path_codes, source_times):
    nv = vectors.shape[0]
    sites = vectors.shape[4]
    size = lax.axis_size("gy")
    y_total = vectors.shape[3] * size
    moms = momenta.shape[0]
    paths = path_codes.shape[0]
    down = [((i + 1) % size, i) for i in range(size)]
    lead = jnp.transpose(vectors, (0, 2, 3, 1, 4))
    lead_up = lax.ppermute(lead, "gy", down)
    links_up = lax.ppermute(gauge_links[1], "gy", down)
    here = jnp.transpose(lead, (0, 3, 1, 2, 4)).reshape(nv, 6 * sites)
    above = jnp.transpose(lead_up, (0, 3, 1, 2, 4)).reshape(nv, 6 * sites)

    link_y = gauge_links[0, :, :, :, 0].astype(F32)
    link_z = gauge_links[1, :, :, :, 0].astype(F32)
    link_z_up = links_up[:, :, :, 0].astype(F32)
    y_here = lax.axis_index("gy")
    links, trig = [], []
    for d in range(paths):
        links.append(path_link(link_y, link_z, link_z_up, path_codes[d]))
        angles = phase_angles(momenta, y_here + jnp.where(path_codes[d, 0] == 1, 0, 1), y_total)
        trig.append(jnp.concatenate([jnp.cos(angles), jnp.sin(angles)]))
    links = jnp.stack(links).reshape(paths, 18, sites)
    trig = jnp.stack(trig)

    rows = nv // size
    steps, planes = paths * moms, size // 4
    norm = 1.0 / math.sqrt(6 * y_total * sites)
    vmem = pl.BlockSpec(memory_space=pltpu.VMEM)
    right = pl.pallas_call(
        functools.partial(fused_kernel, norm, moms),
        out_shape=jax.ShapeDtypeStruct((steps, 2, planes, 2, 2, rows, nv), BF),
        in_specs=[pl.BlockSpec(memory_space=pltpu.SMEM), vmem, vmem, vmem, vmem],
        out_specs=vmem,
        scratch_shapes=[
            pltpu.VMEM((2, nv, 6 * sites), BF),
            pltpu.VMEM((2, nv, 6 * sites), BF),
            pltpu.VMEM((nv, 6 * sites), F32),
            pltpu.VMEM((moms, nv, 6 * sites), BF),
            pltpu.VMEM((steps, 2, planes, 2, 2, rows, nv), BF),
            pltpu.VMEM((steps, 2, planes, 2, rows, nv), BF),
            pltpu.VMEM((steps, 2, planes, rows, nv), BF),
            pltpu.VMEM((steps, 2, planes, rows, nv), F32),
            pltpu.VMEM((steps, 2, planes, rows, nv), BF),
            pltpu.VMEM((steps, 2, planes, rows, nv), BF),
            pltpu.VMEM((steps, planes, 2, rows, nv), BF),
            pltpu.SemaphoreType.DMA((8, steps)),
            pltpu.SemaphoreType.DMA((4, steps, planes)),
        ],
        compiler_params=pltpu.CompilerParams(
            collective_id=0, has_side_effects=True, vmem_limit_bytes=60 * 2**20
        ),
    )(path_codes, links, trig, here, above).reshape(steps, 2 * nv, nv)

    chosen = perambulators[source_times]
    times, spins, sources = chosen.shape[:3]
    own = chosen.shape[4]
    re, im = chosen[:, :, :, 0], chosen[:, :, :, 1]
    left = jnp.stack(
        [jnp.concatenate([re, -im], axis=-1), jnp.concatenate([im, re], axis=-1)], axis=4
    ).reshape(times, spins * sources * own * 2, 2 * nv)
    count = spins * sources * own
    out = pl.pallas_call(
        contract_kernel,
        grid=(times,),
        out_shape=jax.ShapeDtypeStruct((times, count, paths, moms, 2, nv), BF),
        in_specs=[
            pl.BlockSpec((1, 2 * count, 2 * nv), lambda s: (s, 0, 0)),
            pl.BlockSpec((steps, 2 * nv, nv), lambda s: (0, 0, 0)),
        ],
        out_specs=pl.BlockSpec((1, count, paths, moms, 2, nv), lambda s: (s, 0, 0, 0, 0, 0)),
        compiler_params=pltpu.CompilerParams(vmem_limit_bytes=60 * 2**20),
    )(left, right)
    return out.reshape(times, spins, sources, own, paths, moms, 2, nv)


def solution(mesh):
    placed = (
        P("grp", None, None, "gy", None),
        P("grp", None, None, None, "gy", None),
        P("grp", None, None, None, "gy", None),
        P(),
        P(),
        P("grp"),
    )
    return jax.shard_map(
        shards,
        mesh=mesh,
        in_specs=placed,
        out_specs=P("grp", None, None, "gy", None, None, None, None),
        check_vma=False,
    )
```
